32 devices in a mesh: expert: 8 (over z, y), tensor: 4 (over x, core).
Axes of the slice: x: 2, y: 2, z: 4, core: 2. Of those that a mesh axis runs over, the one named last changes fastest.
Arguments:
- tokens: bfloat16 [1024, 3072], P('expert', 'tensor'), may hold values from -6 to 6
- expert_ids: int32 [1024, 2], P('expert'), may hold values from 0 to 7, all different within a row; in each aligned block of 128 rows (0 to 127, 128 to 255, ...) at most 48 rows name the same one
- joined_weight: bfloat16 [8, 3072, 2, 16384], P('expert', 'tensor'), may hold values from -0.109375 to 0.109375
Outputs:
- hidden: bfloat16 [1024, 2, 1, 16384], P('expert', None, None, 'tensor')
The draws below stay inside these ranges and needn't reach their ends.
Inputs may be any that keep to these rules, and one draw needn't show every extreme that they name: `expert_ids`: each row names 2 different experts. Among the rows of one device (each aligned block of 128 rows) no expert is named by more than 48 rows, and in some blocks one expert is named by exactly 48 rows.
All inputs are finite; a program needn't handle non-finite values.
Results may differ from the reference program's by a relative error of at most 0.001.
Values may be sent and summed in bfloat16 or wider, within the bound.
A program may use at most 256 MiB of HBM per device.

```python
import math
import jax
import jax.numpy as jnp
import numpy as np
from jax import lax

E = 8
TOP = 2
D = 3072
FF = 16384
TOK_DEV = 128
CAP = 48
REP = 1
FB = 16384
EB = 8
TOKENS = 1024


def levels(own_key, dims, cuts, low, high):
    loudness = 1.0
    for dim, blocks in cuts:
        steps = jax.random.uniform(jax.random.fold_in(jax.random.fold_in(own_key, 6), dim), (blocks,), jnp.float32, low / len(cuts), high / len(cuts))
        loudness = loudness * jnp.repeat(jnp.exp(steps), dims[dim] // blocks).reshape((-1,) + (1,) * (len(dims) - 1 - dim))
    return loudness


def shared_out(key, own, number, rows, amount, top, bound, lean):
    order = jax.random.permutation(key, amount)
    crowded, usual = load_shares(amount, rows * top, bound, lean, True), load_shares(amount, rows * top, bound, lean, False)
    places = jnp.arange(amount)

    def named(tallies, rotation):
        used = int((tallies > 0).sum())
        fixed = max(1, used // 4)
        passed = fixed + (places - fixed + rotation * (used - fixed)) % max(1, amount - fixed)
        return jnp.zeros((amount,), jnp.int32).at[order[jnp.where(places < fixed, places, passed)]].set(jnp.asarray(tallies, jnp.int32))

    tallies = jnp.where(number % 4 == 0, named(crowded, number // 4), named(usual, number - number // 4 - 1))
    mixed = jax.random.permutation(jax.random.fold_in(own, 3), amount)
    giver, sink = mixed[0:amount // 2 * 2:2], mixed[1:amount // 2 * 2:2]
    margin = jnp.minimum(tallies[giver] - 1, bound - tallies[sink]) // 2
    margin = jnp.where((giver == order[0]) | (sink == order[0]) | (tallies[sink] == 0), 0, jnp.maximum(margin, 0))
    passed = jax.random.randint(jax.random.fold_in(own, 4), (amount // 2,), 0, 1 << 20) % (margin + 1)
    tallies = tallies.at[giver].add(-passed).at[sink].add(passed)
    labels = jnp.searchsorted(jnp.cumsum(tallies), jnp.arange(rows * top), side="right").astype(jnp.int32)
    listing = labels.reshape(top, rows).T
    listing = listing[jax.random.permutation(jax.random.fold_in(own, 1), rows)]
    rotation = jax.random.randint(jax.random.fold_in(own, 2), (rows, 1), 0, top)
    return jnp.take_along_axis(listing, (jnp.arange(top)[None, :] + rotation) % top, axis=1)


def load_shares(amount, total, bound, lean, full):
    portions = [(1 << 20) // math.isqrt(standing ** lean) + 1 for standing in range(1, amount + 1)]
    largest = bound if full else min(bound, max(-(-total // amount), total * portions[0] // sum(portions)))
    least = 1 if total - largest >= amount - 1 else 0
    holding, spare = [largest] + [least] * (amount - 1), total - largest - least * (amount - 1)
    while spare > 0:
        free = [i for i in range(1, amount) if holding[i] < largest] or [i for i in range(1, amount) if holding[i] < bound]
        mass, remaining = sum([portions[i] for i in free]), spare
        for i in free:
            addition = min(bound - holding[i], max(1, remaining * portions[i] // mass), spare)
            holding[i] = holding[i] + addition
            spare = spare - addition
    return np.array(holding)


def gaussian(rng, shape, deviation, reach, split=(), kind=jnp.bfloat16):
    drawn = jax.random.normal(rng, shape, jnp.float32) * deviation
    if len(split) > 0:
        drawn = levels(rng, shape, split, -0.22, 0.18) * drawn
    return jnp.clip(drawn, min=-reach, max=reach).astype(kind)


def setup_inputs(seed: int = 0) -> dict:
    key_of = jax.random.split(jax.random.key(seed), 4)
    tokens = gaussian(key_of[0], (TOKENS, D), 1.0, 6.0, ((0, 8), (1, 4)))
    expert_ids_keys = jax.random.split(jax.random.fold_in(key_of[1], 1), TOKENS // TOK_DEV)
    expert_ids_turns = jax.random.permutation(jax.random.fold_in(key_of[1], 3), TOKENS // TOK_DEV)
    expert_ids = jax.vmap(lambda own, number: shared_out(jax.random.fold_in(key_of[1], 2), own, number, TOK_DEV, E, TOP, CAP, 2))(expert_ids_keys, expert_ids_turns).reshape((TOKENS, TOP))
    joined_weight = gaussian(key_of[2], (EB, D, 2, FB), D ** -0.5, 0.109375, ((0, 8), (1, 4)))
    return {"tokens": tokens, "expert_ids": expert_ids, "joined_weight": joined_weight}


def reference(tokens, expert_ids, joined_weight):
    sources = TOKENS // TOK_DEV
    flat_ids = expert_ids.reshape(sources, TOK_DEV * TOP)
    chosen = (flat_ids[:, :, None] == jnp.arange(E, dtype=jnp.int32)[None, None, :]).astype(jnp.int32)
    earlier = jnp.cumsum(chosen, axis=1) - chosen
    position = jnp.sum(earlier * chosen, axis=2).astype(jnp.int32)
    slot_index = (jnp.arange(sources, dtype=jnp.int32)[:, None] * CAP + position).reshape(-1).astype(jnp.int32)
    all_ids = flat_ids.reshape(-1)
    token_of = (jnp.arange(TOKENS * TOP, dtype=jnp.int32) // TOP).astype(jnp.int32)
    routed = tokens[token_of]

    def one_expert(index, result):
        expert = jnp.asarray(index).astype(jnp.int32)
        w_block = lax.dynamic_slice_in_dim(joined_weight, (expert * REP).astype(jnp.int32), REP, 0)
        weight = jnp.transpose(w_block, (1, 2, 0, 3)).reshape(D, 2 * FF)
        is_mine = all_ids == expert
        target = jnp.where(is_mine, slot_index, sources * CAP).astype(jnp.int32)
        buffer = jnp.zeros((sources * CAP + 1, D), jnp.bfloat16).at[target].set(routed)
        gate_up = jnp.dot(buffer, weight, preferred_element_type=jnp.float32)
        active = (jax.nn.silu(gate_up[:, :FF]) * gate_up[:, FF:]).astype(jnp.bfloat16)
        return jnp.where(is_mine[:, None], active[target], result)

    start_out = jnp.zeros((TOKENS * TOP, FF), jnp.bfloat16)
    result = lax.fori_loop(0, E, one_expert, start_out)
    return result.reshape(TOKENS, TOP, REP, FB)
```

```python
import functools

import jax
import jax.numpy as jnp
from jax import lax
from jax.experimental import pallas as pl
from jax.experimental.pallas import tpu as pltpu
from jax.sharding import PartitionSpec as P

E = 8
TOP = 2
CAP = 48
TOP_CODE = 32767.0
SLOTS = 4
LAG = 2


def remote(src, dst, send, recv, **where):
    return pltpu.make_async_remote_copy(
        src_ref=src,
        dst_ref=dst,
        send_sem=send,
        recv_sem=recv,
        device_id=where,
        device_id_type=pl.DeviceIdType.MESH,
    )


def kernel(
    groups, blocks, half, width, chunk, sub,
    placed, pick, weight, out,
    x, w, part, qs, qr, scale_s, scale_r, base, act, ret, stage,
    tok_send, tok_recv, fwd_send, fwd_recv,
    w_local, w_send, w_recv, q_send, q_recv, s_send, s_recv,
    act_send, act_recv, out_sem, credit,
):
    copies = blocks // E
    chips = groups // 2
    rows = blocks * CAP
    count = half // chunk
    parts = chunk // sub
    subs = half // sub
    far = (chips - 1) * count
    total = chips * count
    e, t = lax.axis_index("expert"), lax.axis_index("tensor")
    core, chip = lax.rem(t, 2), lax.div(t, 2)
    partner = chip * 2 + 1 - core
    tokens = pick.shape[1]

    def peer(d):
        return lax.rem(e + d, blocks)

    def across(o):
        return lax.rem(chip + o, chips) * 2 + core

    barrier = pltpu.get_barrier_semaphore()

    def greet(**where):
        pl.semaphore_signal(barrier, inc=1, device_id=where, device_id_type=pl.DeviceIdType.MESH)

    for d in range(1, blocks):
        greet(expert=peer(d))
    greet(tensor=partner)
    for o in range(1, chips):
        greet(tensor=across(o))
    pl.semaphore_wait(barrier, blocks - 1 + 1 + chips - 1)

    def bring(k, slot):
        target = lax.rem(chip + 1 + lax.div(k, count), chips)
        j = lax.rem(k, count)
        mine = pl.multiple_of((target * 2 + core) * half + j * chunk, 128)
        theirs = pl.multiple_of((target * 2 + 1 - core) * half + j * chunk, 128)
        here = pltpu.make_async_copy(
            weight.at[0, :, :, pl.ds(mine, chunk)], w.at[slot, 0], w_local.at[slot]
        )
        there = remote(
            weight.at[0, :, :, pl.ds(theirs, chunk)], w.at[slot, 1],
            w_send.at[slot], w_recv.at[slot], tensor=partner,
        )
        return here, there

    def start_weights(k, slot):
        here, there = bring(k, slot)
        there.start()
        here.start()

    token_copies = []
    for d in range(1, blocks):
        copy = remote(
            placed.at[lax.div(peer(d), copies)], x.at[0, e],
            tok_send.at[d], tok_recv.at[e], expert=peer(d),
        )
        copy.start()
        token_copies.append(copy)
    for k in range(min(SLOTS, total)):
        start_weights(k, k)
    x[0, e] = placed[lax.div(e, copies)]

    forwards = []
    for d in range(blocks):
        source = lax.rem(e + blocks - d, blocks)
        src = x.at[0, source]
        if d == 0:
            src = placed.at[lax.div(e, copies)]
        else:
            remote(
                x.at[0, source], x.at[0, source], tok_send.at[0], tok_recv.at[source],
                expert=source,
            ).wait_recv()
        copy = remote(
            src, x.at[1, source], fwd_send.at[source], fwd_recv.at[source], tensor=partner
        )
        copy.start()
        forwards.append(copy)
    for copy in forwards:
        copy.wait_recv()

    def products(k, use):
        slot = lax.rem(k, SLOTS)
        here, there = bring(k, slot)
        here.wait()
        there.wait_recv()
        own = x[0].reshape(rows, width)
        other = x[1].reshape(rows, width)
        mine = jnp.swapaxes(w[slot, 0], 0, 1)
        theirs = jnp.swapaxes(w[slot, 1], 0, 1)
        for c in range(2):
            use(
                c,
                jnp.dot(own, mine[c], preferred_element_type=jnp.float32)
                + jnp.dot(other, theirs[c], preferred_element_type=jnp.float32),
            )

        @pl.when(k + SLOTS < total)
        def _():
            pl.semaphore_signal(
                credit, inc=1, device_id={"tensor": partner}, device_id_type=pl.DeviceIdType.MESH
            )

        @pl.when(jnp.logical_and(k >= 1, k - 1 + SLOTS < total))
        def _():
            before = lax.rem(k + SLOTS - 1, SLOTS)
            bring(k - 1, before)[1].wait_send()
            pl.semaphore_wait(credit, 1)
            start_weights(k - 1 + SLOTS, before)

    def code_copies(o, q):
        return (
            remote(qs.at[q], qr.at[q], q_send.at[q], q_recv.at[q], tensor=across(o)),
            remote(scale_s.at[q], scale_r.at[q], s_send.at[q], s_recv.at[q], tensor=across(o)),
        )

    def far_step(k, carry):
        def use(c, value):
            part[c] = value

        products(k, use)
        o = 1 + lax.div(k, count)
        j = lax.rem(k, count)
        for h in range(parts):
            q = (o - 1) * subs + j * parts + h
            for c in range(2):
                value = part[c, :, h * sub : (h + 1) * sub]
                top = jnp.maximum(jnp.max(jnp.abs(value), axis=0, keepdims=True), 1e-30)
                code = jnp.round(value * (TOP_CODE / top)).astype(jnp.int32).astype(jnp.int16)
                qs[q, :, c * sub : (c + 1) * sub] = code
                scale_s[q, :, c * sub : (c + 1) * sub] = top * (1.0 / TOP_CODE)
            for copy in code_copies(o, q):
                copy.start()
        return carry

    def near_step(k, carry):
        j = lax.rem(k, count)

        def use(c, value):
            for h in range(parts):
                base[j * parts + h, c] = value[:, h * sub : (h + 1) * sub]

        products(k, use)
        return carry

    lax.fori_loop(0, far, far_step, 0)
    lax.fori_loop(far, total, near_step, 0)

    def act_copy(s, d):
        return remote(
            act.at[s, peer(d)], ret.at[s, lax.rem(e, copies), lax.div(e, copies)],
            act_send.at[s], act_recv.at[s], expert=peer(d),
        )

    def act_all(s):
        every = act.at[s, pl.ds(0, blocks - 1)]
        return remote(every, every, act_send.at[s], act_recv.at[s], expert=peer(1))

    def out_copy(s):
        return pltpu.make_async_copy(
            stage.at[s], out.at[:, :, :, pl.ds(pl.multiple_of(s * sub, 128), sub)], out_sem.at[s]
        )

    def finish(s):
        act_all(s).wait_recv()
        for r in range(copies):
            got = ret[s, r].reshape(E * CAP, sub)
            picked = [
                jnp.dot(pick[k], got, preferred_element_type=jnp.float32).astype(jnp.bfloat16)
                for k in range(TOP)
            ]
            stage[s, :, r] = jnp.swapaxes(jnp.stack(picked), 0, 1)
        out_copy(s).start()

    def receive(s, carry):
        for o in range(1, chips):
            for copy in code_copies(o, (o - 1) * subs + s):
                copy.wait_recv()
        for b in range(blocks):
            line = slice(b * CAP, (b + 1) * CAP)
            gate, up = base[s, 0, line], base[s, 1, line]
            for o in range(1, chips):
                q = (o - 1) * subs + s
                gate = gate + qr[q, line, :sub].astype(jnp.int32).astype(jnp.float32) * scale_r[q, :, :sub]
                up = up + qr[q, line, sub:].astype(jnp.int32).astype(jnp.float32) * scale_r[q, :, sub:]
            act[s, b] = (gate / (1.0 + jnp.exp(-gate)) * up).astype(jnp.bfloat16)
        for d in range(1, blocks):
            act_copy(s, d).start()
        ret[s, lax.rem(e, copies), lax.div(e, copies)] = act[s, e]

        @pl.when(s >= LAG)
        def _():
            finish(s - LAG)

        return carry

    lax.fori_loop(0, subs, receive, 0)
    for s in range(max(0, subs - LAG), subs):
        finish(s)

    for copy in token_copies:
        copy.wait_send()
    for copy in forwards:
        copy.wait_send()
    for k in range(max(0, total - SLOTS), total):
        bring(k, k % SLOTS)[1].wait_send()
    for o in range(1, chips):

        def sent(s, carry):
            for copy in code_copies(o, (o - 1) * subs + s):
                copy.wait_send()
            return carry

        lax.fori_loop(0, subs, sent, 0)

    def done(s, carry):
        act_all(s).wait_send()
        out_copy(s).wait()
        return carry

    lax.fori_loop(0, subs, done, 0)


def local(tokens, expert_ids, joined_weight):
    groups = lax.axis_size("tensor")
    blocks = lax.axis_size("expert")
    copies = blocks // E
    chips = groups // 2
    half = joined_weight.shape[3] // groups
    tok_count, width = tokens.shape
    chunk = 512 if half % 512 == 0 else half
    sub = 256 if chunk % 256 == 0 else chunk
    subs = half // sub
    rows = blocks * CAP
    codes = (chips - 1) * subs

    flat_ids = expert_ids.reshape(-1)
    chosen = (flat_ids[:, None] == jnp.arange(E, dtype=jnp.int32)[None, :]).astype(jnp.int32)
    earlier = jnp.cumsum(chosen, axis=0) - chosen
    position = jnp.sum(earlier * chosen, axis=1)
    slot_index = flat_ids * CAP + position
    pick = (slot_index[:, None] == jnp.arange(E * CAP, dtype=jnp.int32)[None, :]).astype(
        jnp.bfloat16
    )
    pick = pick.reshape(tok_count, TOP, E * CAP)
    placed = lax.dot_general(
        pick.sum(axis=1), tokens, (((0,), (0,)), ((), ())), preferred_element_type=jnp.float32
    )
    placed = placed.astype(jnp.bfloat16).reshape(E, CAP, width)
    pick = pick.transpose(1, 0, 2)

    dma = pltpu.SemaphoreType.DMA
    vmem = pl.BlockSpec(memory_space=pltpu.VMEM)
    hbm = pl.BlockSpec(memory_space=pl.ANY)
    result = pl.pallas_call(
        functools.partial(kernel, groups, blocks, half, width, chunk, sub),
        out_shape=jax.ShapeDtypeStruct((tok_count, copies, TOP, half), jnp.bfloat16),
        in_specs=[vmem, vmem, hbm],
        out_specs=hbm,
        scratch_shapes=[
            pltpu.VMEM((2, blocks, CAP, width), jnp.bfloat16),
            pltpu.VMEM((SLOTS, 2, width, 2, chunk), jnp.bfloat16),
            pltpu.VMEM((2, rows, chunk), jnp.float32),
            pltpu.VMEM((codes, rows, 2 * sub), jnp.int16),
            pltpu.VMEM((codes, rows, 2 * sub), jnp.int16),
            pltpu.VMEM((codes, 1, 2 * sub), jnp.float32),
            pltpu.VMEM((codes, 1, 2 * sub), jnp.float32),
            pltpu.VMEM((subs, 2, rows, sub), jnp.float32),
            pltpu.VMEM((subs, blocks, CAP, sub), jnp.bfloat16),
            pltpu.VMEM((subs, copies, E, CAP, sub), jnp.bfloat16),
            pltpu.VMEM((subs, tok_count, copies, TOP, sub), jnp.bfloat16),
            dma((blocks,)), dma((blocks,)), dma((blocks,)), dma((blocks,)),
            dma((SLOTS,)), dma((SLOTS,)), dma((SLOTS,)),
            dma((codes,)), dma((codes,)), dma((codes,)), dma((codes,)),
            dma((subs,)), dma((subs,)), dma((subs,)),
            pltpu.SemaphoreType.REGULAR,
        ],
        compiler_params=pltpu.CompilerParams(
            collective_id=0, has_side_effects=True, vmem_limit_bytes=66 * 1024 * 1000
        ),
        name="experts",
    )(placed, pick, joined_weight)
    return result.transpose(0, 2, 1, 3)


def solution(mesh):
    placed = (P("expert", "tensor"), P("expert", None), P("expert", "tensor", None, None))
    return jax.shard_map(
        local,
        mesh=mesh,
        in_specs=placed,
        out_specs=P("expert", None, None, "tensor"),
        check_vma=False,
    )
```

```python
import functools

import jax
import jax.numpy as jnp
from jax import lax
from jax.experimental import pallas as pl
from jax.experimental.pallas import tpu as pltpu
from jax.sharding import PartitionSpec as P

E = 8
TOP = 2
CAP = 48
TOP_CODE = 32767.0
SLOTS = 6
OPEN = 5
SPLIT = 3
LAST = 2
MESH = pl.DeviceIdType.MESH


def remote(src, dst, send, recv, **where):
    return pltpu.make_async_remote_copy(
        src_ref=src,
        dst_ref=dst,
        send_sem=send,
        recv_sem=recv,
        device_id=where,
        device_id_type=MESH,
    )


def flipped(index, distance):
    bit = 1
    while bit <= distance:
        if distance & bit:
            index = index + bit - 2 * bit * lax.rem(lax.div(index, bit), 2)
        bit *= 2
    return index


def kernel(
    groups, blocks, half, width, chunk,
    tokens, ids, weight, out,
    tok_v, ids_v, placed, pick, x, w, qs, qr, scale_s, scale_r, base, act, ret, stage,
    in_sem, tok_send, tok_recv, fwd_send, fwd_recv,
    w_local, w_send, w_recv, q_send, q_recv, s_send, s_recv,
    act_send, act_recv, out_sem, credit,
):
    copies = blocks // E
    chips = groups // 2
    near = blocks // 2
    count = half // chunk
    far = (chips - 1) * count
    total = chips * count
    e, t = lax.axis_index("expert"), lax.axis_index("tensor")
    core, chip = lax.rem(t, 2), lax.div(t, 2)
    partner = chip * 2 + 1 - core
    tok_count = tok_v.shape[0]
    peers = [flipped(e, d) for d in range(blocks)]

    def across(o):
        return lax.rem(chip + o, chips) * 2 + core

    barrier = pltpu.get_barrier_semaphore()

    def greet(**where):
        pl.semaphore_signal(barrier, inc=1, device_id=where, device_id_type=MESH)

    ids_in = pltpu.make_async_copy(ids, ids_v, in_sem.at[0])
    tokens_in = pltpu.make_async_copy(tokens, tok_v, in_sem.at[1])
    ids_in.start()
    tokens_in.start()
    for d in range(1, blocks):
        greet(expert=peers[d])
    greet(tensor=partner)
    for o in range(1, chips):
        greet(tensor=across(o))

    opening = min(OPEN, far)
    split = min(SPLIT, opening)
    last = min(LAST, far - opening)
    mixed = chips == 2 and count > OPEN + LAST
    middle = far - opening - last if mixed else 0

    def own_apart(k):
        return jnp.logical_or(k < split, k >= far - last)

    def piece(n):
        if not mixed:
            return n
        m = n - opening
        turn = jnp.where(lax.rem(m, 2) == 0, opening + lax.div(m, 2), far + lax.div(m, 2))
        rest = jnp.where(m < 2 * middle + last, opening + m - middle, far + m - middle - last)
        return jnp.where(m < 0, n, jnp.where(m < 2 * middle, turn, rest))

    def bring(n, slot):
        k = piece(n)
        target = lax.rem(chip + 1 + lax.div(k, count), chips)
        j = lax.rem(k, count)
        mine = pl.multiple_of((target * 2 + core) * half + j * chunk, 128)
        theirs = pl.multiple_of((target * 2 + 1 - core) * half + j * chunk, 128)
        here = pltpu.make_async_copy(
            weight.at[0, :, :, pl.ds(mine, chunk)], w.at[slot, 0], w_local.at[slot]
        )
        there = remote(
            weight.at[0, :, :, pl.ds(theirs, chunk)], w.at[slot, 1],
            w_send.at[slot], w_recv.at[slot], tensor=partner,
        )
        return here, there

    ahead = min(SLOTS, total)
    for k in range(ahead):
        bring(k, k)[0].start()

    pl.semaphore_wait(barrier, blocks - 1 + 1 + chips - 1)
    bring(0, 0)[1].start()

    ids_in.wait()
    named = lax.broadcasted_iota(jnp.int32, (E, tok_count), 0)
    chosen = [(named == ids_v[k : k + 1, :]).astype(jnp.float32) for k in range(TOP)]
    before = lax.broadcasted_iota(jnp.int32, (tok_count, tok_count), 0) < lax.broadcasted_iota(
        jnp.int32, (tok_count, tok_count), 1
    )
    seen = jnp.dot(
        sum(chosen).astype(jnp.bfloat16),
        before.astype(jnp.float32).astype(jnp.bfloat16),
        preferred_element_type=jnp.float32,
    )
    line = lax.broadcasted_iota(jnp.int32, (E * CAP, tok_count), 0)
    taken = []
    for k in range(TOP):
        position = jnp.sum(seen * chosen[k], axis=0, keepdims=True).astype(jnp.int32)
        taken.append((line == ids_v[k : k + 1, :] * CAP + position).astype(jnp.float32))
        seen = seen + chosen[k]
    tokens_in.wait()
    placed[...] = (
        jnp.dot(sum(taken).astype(jnp.bfloat16), tok_v[...], preferred_element_type=jnp.float32)
        .astype(jnp.bfloat16)
        .reshape(E, CAP, width)
    )

    def token_copy(d):
        return remote(
            placed.at[lax.div(peers[d], copies)], x.at[0, d],
            tok_send.at[d], tok_recv.at[d], expert=peers[d],
        )

    def forward(d):
        src = x.at[0, d] if d else placed.at[lax.div(e, copies)]
        return remote(src, x.at[1, d], fwd_send.at[d], fwd_recv.at[d], tensor=partner)

    forward(0).start()
    for d in range(1, near):
        token_copy(d).start()
    for k in range(1, min(SPLIT, ahead)):
        bring(k, k)[1].start()
    x[0, 0] = placed[lax.div(e, copies)]

    def products(slot, first, some, use):
        own = x[0, pl.ds(first, some)].reshape(some * CAP, width)
        other = x[1, pl.ds(first, some)].reshape(some * CAP, width)
        mine = jnp.swapaxes(w[slot, 0], 0, 1)
        theirs = jnp.swapaxes(w[slot, 1], 0, 1)
        for c in range(2):
            use(
                c,
                jnp.dot(own, mine[c], preferred_element_type=jnp.float32)
                + jnp.dot(other, theirs[c], preferred_element_type=jnp.float32),
            )

    def await_weights(k):
        here, there = bring(k, lax.rem(k, SLOTS))
        here.wait()
        there.wait_recv()

    def release(k):
        @pl.when(k + SLOTS < total)
        def _():
            pl.semaphore_signal(credit, inc=1, device_id={"tensor": partner}, device_id_type=MESH)

        @pl.when(jnp.logical_and(k >= 1, k - 1 + SLOTS < total))
        def _():
            old = lax.rem(k + SLOTS - 1, SLOTS)
            here, there = bring(k - 1 + SLOTS, old)
            there.wait_send()
            pl.semaphore_wait(credit, 1)
            there.start()
            here.start()

    def code_copies(k, at, first, some):
        o = 1 + lax.div(k, count)
        span = pl.ds(pl.multiple_of(first * CAP, 16), some * CAP)
        return (
            remote(qs.at[k, span], qr.at[k, span], q_send.at[at, k], q_recv.at[at, k], tensor=across(o)),
            remote(scale_s.at[at, k], scale_r.at[at, k], s_send.at[at, k], s_recv.at[at, k], tensor=across(o)),
        )

    def send(n, k, at, first, some):
        def use(c, value):
            top = jnp.maximum(jnp.max(jnp.abs(value), axis=0, keepdims=True), 1e-30)
            code = jnp.round(value * (TOP_CODE / top)).astype(jnp.int32).astype(jnp.int16)
            span = pl.ds(pl.multiple_of(first * CAP, 16), some * CAP)
            qs[k, span, c * chunk : (c + 1) * chunk] = code
            scale_s[at, k, :, c * chunk : (c + 1) * chunk] = top * (1.0 / TOP_CODE)

        products(lax.rem(n, SLOTS), first, some, use)
        for copy in code_copies(k, at, first, some):
            copy.start()

    def own_step(k, carry):
        await_weights(k)
        send(k, k, 2, 0, 1)
        return carry

    def near_rows(k, carry):
        send(k, k, 0, 1, near - 1)
        return carry

    def near_part(k, carry):
        await_weights(k)
        send(k, k, 0, 0, near)
        return carry

    def far_part(k, carry):
        send(k, k, 1, near, blocks - near)
        release(k)
        return carry

    def both(n, k):
        await_weights(n)

        def half_of_rows(i, carry):
            r = 1 - i
            send(n, k, r, r * near, near)
            return carry

        lax.fori_loop(0, 2, half_of_rows, 0)
        release(n)

    def others(i, carry):
        n = opening + 2 * middle + i if mixed else far - last + i
        await_weights(n)
        send(n, far - last + i, 1, near, blocks - near)
        send(n, far - last + i, 0, 1, near - 1)
        return carry

    def own_late(i, carry):
        n = opening + 2 * middle + i if mixed else far - last + i
        send(n, far - last + i, 2, 0, 1)
        release(n)
        return carry

    def own_chip(n, j):
        await_weights(n)

        def use(c, value):
            base[lax.rem(j, base.shape[0]), c] = value

        products(lax.rem(n, SLOTS), 0, blocks, use)
        release(n)

    forward(0).wait_recv()
    lax.fori_loop(0, min(1, split), own_step, 0)
    for d in range(1, near):
        token_copy(d).wait_recv()
        forward(d).start()
    for d in range(near, blocks):
        token_copy(d).start()
    for k in range(split, min(opening, ahead)):
        bring(k, k)[1].start()
    lax.fori_loop(1, split, own_step, 0)
    for d in range(1, near):
        forward(d).wait_recv()
    lax.fori_loop(0, split, near_rows, 0)
    lax.fori_loop(split, opening, near_part, 0)
    for k in range(TOP):
        pick[k] = taken[k].T.astype(jnp.bfloat16)
    for d in range(near, blocks):
        token_copy(d).wait_recv()
        forward(d).start()
    for k in range(opening, ahead):
        bring(k, k)[1].start()
    for d in range(near, blocks):
        forward(d).wait_recv()
    lax.fori_loop(0, opening, far_part, 0)
    def act_copy(s, d):
        return remote(
            act.at[s, d], ret.at[s, lax.rem(e, copies), lax.div(e, copies)],
            act_send.at[s], act_recv.at[s], expert=peers[d],
        )

    def act_all(s):
        every = act.at[s, pl.ds(0, blocks - 1)]
        return remote(every, every, act_send.at[s], act_recv.at[s], expert=peers[1])

    def out_copy(s):
        return pltpu.make_async_copy(
            stage.at[s], out.at[:, :, :, pl.ds(pl.multiple_of(s * chunk, 128), chunk)], out_sem.at[s]
        )

    def finish(s, carry):
        act_all(s).wait_recv()
        for r in range(copies):
            got = ret[s, r].reshape(E * CAP, chunk)
            picked = [
                jnp.dot(pick[k], got, preferred_element_type=jnp.float32).astype(jnp.bfloat16)
                for k in range(TOP)
            ]
            stage[s, :, r] = jnp.swapaxes(jnp.stack(picked), 0, 1)
        out_copy(s).start()
        return carry

    def activate(s, b):
        line = slice(b * CAP, (b + 1) * CAP)
        at = lax.rem(s, base.shape[0])
        gate, up = base[at, 0, line], base[at, 1, line]
        for o in range(1, chips):
            k = (o - 1) * count + s
            at = b // near if b else jnp.where(own_apart(k), 2, 0)
            scale = scale_r[at, k]
            gate = gate + qr[k, line, :chunk].astype(jnp.int32).astype(jnp.float32) * scale[:, :chunk]
            up = up + qr[k, line, chunk:].astype(jnp.int32).astype(jnp.float32) * scale[:, chunk:]
        return (gate / (1.0 + jnp.exp(-gate)) * up).astype(jnp.bfloat16)

    def hand_back(s, first, end):
        for d in range(first, end):
            act[s, d] = activate(s, d)
            act_copy(s, d).start()

    def keep(s):
        ret[s, lax.rem(e, copies), lax.div(e, copies)] = activate(s, 0)

    def await_codes(k, at, first, some):
        for copy in code_copies(k, at, first, some):
            copy.wait_recv()

    def await_near(k):
        @pl.when(own_apart(k))
        def _():
            await_codes(k, 2, 0, 1)
            await_codes(k, 0, 1, near - 1)

        @pl.when(jnp.logical_not(own_apart(k)))
        def _():
            await_codes(k, 0, 0, near)

    def whole(s, carry):
        for o in range(1, chips):
            k = (o - 1) * count + s
            await_codes(k, 1, near, blocks - near)
            await_near(k)
        hand_back(s, 1, blocks)
        keep(s)
        return carry

    def nearer(s, carry):
        await_near(s)
        hand_back(s, 1, near)
        keep(s)
        return carry

    def farther(s, carry):
        await_codes(s, 1, near, blocks - near)
        hand_back(s, near, blocks)
        return carry

    def received(s):
        farther(s, 0)

        @pl.when(s >= 2)
        def _():
            finish(s - 2, 0)

        nearer(s, 0)

    def turn(i, carry):
        both(opening + 2 * i, opening + i)
        own_chip(opening + 2 * i + 1, i)
        received(i)
        return carry

    def drain(i, carry):
        own_chip(far + i, i)
        received(i)
        return carry

    def received_last(s, carry):
        own_chip(far + s, s)
        farther(s, 0)
        finish(s - 2, 0)
        await_codes(s, 0, 1, near - 1)
        hand_back(s, 1, near)
        return carry

    def received_own(s, carry):
        await_codes(s, 2, 0, 1)
        keep(s)
        return finish(s, 0)

    if mixed:
        lax.fori_loop(0, middle, turn, 0)
        lax.fori_loop(0, last, others, 0)
        lax.fori_loop(0, last, own_late, 0)
        lax.fori_loop(middle, count - last, drain, 0)
        lax.fori_loop(count - last, count, received_last, 0)
        lax.fori_loop(count - last, count, received_own, 0)
    else:

        def sent_whole(k, carry):
            both(k, k)
            return carry

        def own_whole(j, carry):
            own_chip(far + j, j)
            return carry

        lax.fori_loop(opening, far - last, sent_whole, 0)
        lax.fori_loop(0, last, others, 0)
        lax.fori_loop(0, last, own_late, 0)
        lax.fori_loop(0, count, own_whole, 0)
        lax.fori_loop(0, count, whole, 0)
        lax.fori_loop(0, count, finish, 0)

    for d in range(1, blocks):
        token_copy(d).wait_send()
    for d in range(blocks):
        forward(d).wait_send()
    for k in range(max(0, total - SLOTS), total):
        bring(k, k % SLOTS)[1].wait_send()

    def sent(k, carry):
        for copy in code_copies(k, 1, near, blocks - near):
            copy.wait_send()

        @pl.when(own_apart(k))
        def _():
            for copy in code_copies(k, 0, 1, near - 1) + code_copies(k, 2, 0, 1):
                copy.wait_send()

        @pl.when(jnp.logical_not(own_apart(k)))
        def _():
            for copy in code_copies(k, 0, 0, near):
                copy.wait_send()

        return carry

    lax.fori_loop(0, far, sent, 0)

    def done(s, carry):
        act_all(s).wait_send()
        out_copy(s).wait()
        return carry

    lax.fori_loop(0, count, done, 0)


def local(tokens, expert_ids, joined_weight):
    groups = lax.axis_size("tensor")
    blocks = lax.axis_size("expert")
    copies = blocks // E
    chips = groups // 2
    half = joined_weight.shape[3] // groups
    tok_count, width = tokens.shape
    chunk = 256 if half % 256 == 0 else half
    count = half // chunk
    rows = blocks * CAP
    codes = (chips - 1) * count

    dma = pltpu.SemaphoreType.DMA
    hbm = pl.BlockSpec(memory_space=pl.ANY)
    result = pl.pallas_call(
        functools.partial(kernel, groups, blocks, half, width, chunk),
        out_shape=jax.ShapeDtypeStruct((tok_count, copies, TOP, half), jnp.bfloat16),
        in_specs=[hbm, hbm, hbm],
        out_specs=hbm,
        scratch_shapes=[
            pltpu.VMEM((tok_count, width), jnp.bfloat16),
            pltpu.VMEM((TOP, tok_count), jnp.int32),
            pltpu.VMEM((E, CAP, width), jnp.bfloat16),
            pltpu.VMEM((TOP, tok_count, E * CAP), jnp.bfloat16),
            pltpu.VMEM((2, blocks, CAP, width), jnp.bfloat16),
            pltpu.VMEM((SLOTS, 2, width, 2, chunk), jnp.bfloat16),
            pltpu.VMEM((codes, rows, 2 * chunk), jnp.int16),
            pltpu.VMEM((codes, rows, 2 * chunk), jnp.int16),
            pltpu.VMEM((3, codes, 1, 2 * chunk), jnp.float32),
            pltpu.VMEM((3, codes, 1, 2 * chunk), jnp.float32),
            pltpu.VMEM((2 if chips == 2 and count > OPEN + LAST else count, 2, rows, chunk), jnp.float32),
            pltpu.VMEM((count, blocks, CAP, chunk), jnp.bfloat16),
            pltpu.VMEM((count, copies, E, CAP, chunk), jnp.bfloat16),
            pltpu.VMEM((count, tok_count, copies, TOP, chunk), jnp.bfloat16),
            dma((2,)), dma((blocks,)), dma((blocks,)), dma((blocks,)), dma((blocks,)),
            dma((SLOTS,)), dma((SLOTS,)), dma((SLOTS,)),
            dma((3, codes)), dma((3, codes)), dma((3, codes)), dma((3, codes)),
            dma((count,)), dma((count,)), dma((count,)),
            pltpu.SemaphoreType.REGULAR,
        ],
        compiler_params=pltpu.CompilerParams(
            collective_id=0, has_side_effects=True, vmem_limit_bytes=51 * 1024 * 1024
        ),
        name="experts",
    )(tokens, expert_ids.T, joined_weight)
    return result.transpose(0, 2, 1, 3)


def solution(mesh):
    placed = (P("expert", "tensor"), P("expert", None), P("expert", "tensor", None, None))
    return jax.shard_map(
        local,
        mesh=mesh,
        in_specs=placed,
        out_specs=P("expert", None, None, "tensor"),
        check_vma=False,
    )
```
